32 devices in a mesh: dp: 4 (over x, core), fsdp: 2 (over y), tensor: 4 (over z).
Axes of the slice: x: 2, y: 2, z: 4, core: 2. Of those that a mesh axis runs over, the one named last changes fastest.
Arguments:
- tokens: bfloat16 [8, 768, 8192], P(('dp', 'fsdp'), 'tensor'), may hold values from -6 to 6
- norm_gain: float32 [8192], replicated, may hold values from 0.85 to 4
- w_qkv: bfloat16 [8192, 5120], P(('dp', 'fsdp'), 'tensor'), may hold values from -0.3 to 0.3
- a_query: bfloat16 [8192, 16], replicated, may hold values from -0.0625 to 0.0625
- query_up_adapter: bfloat16 [16, 4096], P(None, 'tensor'), may hold values from -1.5 to 1.5
- a_value: bfloat16 [8192, 16], replicated, may hold values from -0.0625 to 0.0625
- value_up_adapter: bfloat16 [16, 512], P(None, 'tensor'), may hold values from -1.5 to 1.5
- out_grad: bfloat16 [8, 768, 4096], P(('dp', 'fsdp'), 'tensor'), may hold values from -6 to 6
Outputs:
- attn_out: bfloat16 [8, 768, 4096], P(('dp', 'fsdp'), 'tensor')
- grad_a_query: float32 [8192, 16], replicated
- grad_b_query: float32 [16, 4096], P(None, 'tensor')
- grad_a_value: float32 [8192, 16], replicated
- grad_b_value: float32 [16, 512], P(None, 'tensor')
The draws below stay inside these ranges and needn't reach their ends.
All inputs are finite; a program needn't handle non-finite values.
Results may differ from the reference program's by a relative error of at most 0.015.
The reference program's roundings to bfloat16 on the way count: a program that leaves them out, or rounds other values in their place, can miss the bound.
Values may be sent and summed in bfloat16 or wider, within the bound.
A program may use at most 256 MiB of HBM per device.

```python
import math
import jax
import jax.numpy as jnp
from jax import lax

D = 8192
KV = 4
HD = 128
RANK = 16
QUERY_PER_KV = 8
SEQ = 768
BATCH = 8
QCOLS = 4096
QKV = 5120


WEIGHT_EDGE = 0.296875


def draw_norm_gain(key, part):
    return 1.0 + 0.15 * jax.random.uniform(key, (D,), jnp.float32, -1.0, 1.0)


def draw_tokens(key, part):
    base = jax.random.normal(jax.random.fold_in(key, 11), (BATCH, SEQ, D), jnp.float32)
    return jnp.clip(base, -6.0, 6.0).astype(jnp.bfloat16)


def draw_w_qkv(key, part):
    base = jax.random.normal(jax.random.fold_in(key, 21), (D, QKV), jnp.float32) * (1.0 / math.sqrt(D))
    return jnp.clip(base, -WEIGHT_EDGE, WEIGHT_EDGE).astype(jnp.bfloat16)


def steps_of(stream_key, shape, pieces, least, largest):
    gain = 1.0
    for position, parts in pieces:
        heights = jax.random.uniform(jax.random.fold_in(jax.random.fold_in(stream_key, 6), position), (parts,), jnp.float32, least / len(pieces), largest / len(pieces))
        gain = gain * jnp.repeat(jnp.exp(heights), shape[position] // parts).reshape((-1,) + (1,) * (len(shape) - 1 - position))
    return gain


def normal_values(stream_key, extent, width, bound, shards=(), kind=jnp.bfloat16):
    loudness = steps_of(stream_key, extent, shards, -0.22, 0.18) if shards else 1.0
    drawn = jax.random.normal(stream_key, extent, jnp.float32) * width * loudness
    return jnp.minimum(jnp.maximum(drawn, -bound), bound).astype(kind)


def setup_inputs(seed: int = 0) -> dict:
    keys = jax.random.split(jax.random.key(seed), 9)
    tokens = draw_tokens(jax.random.fold_in(keys[8], 71), 0)
    norm_gain = draw_norm_gain(jax.random.fold_in(keys[8], 71), 0)
    w_qkv = draw_w_qkv(jax.random.fold_in(keys[8], 71), 0)
    a_query = normal_values(keys[3], (D, RANK), D ** -0.5, 0.0625)
    query_up_adapter = normal_values(keys[4], (RANK, QCOLS), RANK ** -0.5, 1.5, ((1, 4),))
    a_value = normal_values(keys[5], (D, RANK), D ** -0.5, 0.0625)
    value_up_adapter = normal_values(keys[6], (RANK, KV * HD), RANK ** -0.5, 1.5, ((1, 4),))
    out_grad = normal_values(keys[7], (BATCH, SEQ, QCOLS), 1.0, 6.0, ((0, 8), (1, 4)))
    return {"tokens": tokens, "norm_gain": norm_gain, "w_qkv": w_qkv, "a_query": a_query, "query_up_adapter": query_up_adapter, "a_value": a_value, "value_up_adapter": value_up_adapter, "out_grad": out_grad}


EPSILON = 1e-05
ADAPTER_SCALE = 2.0
ROPE_BASE = 500000.0

def normalize(own_rows, norm_gain):
    widened = own_rows.astype(jnp.float32)
    mean_square = lax.optimization_barrier(jnp.mean(widened * widened, axis=-1, keepdims=True))
    return (widened * lax.rsqrt(mean_square + EPSILON) * norm_gain).astype(jnp.bfloat16)

def rotary(heads_block):
    sequence_length = heads_block.shape[0]
    half_dim = heads_block.shape[-1] // 2
    positions = jnp.arange(sequence_length, dtype=jnp.float32)[:, None]
    inv_freq = ROPE_BASE ** (-jnp.arange(half_dim, dtype=jnp.float32) / half_dim)
    angles = positions * inv_freq
    cosine = jnp.cos(angles)[:, None, :]
    sine_table = jnp.sin(angles)[:, None, :]
    front_half = heads_block[..., :half_dim].astype(jnp.float32)
    back_half = heads_block[..., half_dim:].astype(jnp.float32)
    turned = jnp.concatenate([front_half * cosine - back_half * sine_table, back_half * cosine + front_half * sine_table], -1)
    return turned.astype(jnp.bfloat16)

def attend(query_rows, key_heads, value_rows):
    sequence_length = query_rows.shape[0]
    kv_heads = key_heads.shape[1] // HD
    rot_queries = rotary(query_rows.reshape(sequence_length, kv_heads * QUERY_PER_KV, HD))
    rot_keys = rotary(key_heads.reshape(sequence_length, kv_heads, HD))
    split_values = value_rows.reshape(sequence_length, kv_heads, HD)
    causal = jnp.arange(sequence_length)[:, None] >= jnp.arange(sequence_length)[None, :]

    def one_head(head_index):
        q_head = lax.dynamic_index_in_dim(rot_queries, head_index, 1, keepdims=False)
        k_head = lax.dynamic_index_in_dim(rot_keys, head_index // QUERY_PER_KV, 1, keepdims=False)
        v_head = lax.dynamic_index_in_dim(split_values, head_index // QUERY_PER_KV, 1, keepdims=False)
        scores = jnp.dot(q_head, k_head.T, preferred_element_type=jnp.float32) * (1.0 / math.sqrt(HD))
        scores = jnp.where(causal, scores, -1e+30)
        row_max = lax.optimization_barrier(jnp.max(scores, axis=-1, keepdims=True))
        weights = jnp.exp(scores - row_max)
        probabilities = (weights / lax.optimization_barrier(jnp.sum(weights, axis=-1, keepdims=True))).astype(jnp.bfloat16)
        return jnp.dot(probabilities, v_head, preferred_element_type=jnp.float32).astype(jnp.bfloat16)
    per_head = lax.map(one_head, jnp.arange(kv_heads * QUERY_PER_KV, dtype=jnp.int32))
    return jnp.transpose(per_head, (1, 0, 2)).reshape(sequence_length, kv_heads * QUERY_PER_KV * HD)

def reference(tokens, norm_gain, w_qkv, a_query, query_up_adapter, a_value, value_up_adapter, out_grad):
    adapters = jnp.concatenate([a_query, a_value], 1)
    narrow_rank_rows = a_query.shape[1]

    def one_sequence(pair):
        own_rows, grad_rows = pair
        normed_input = normalize(own_rows, norm_gain)
        sequence_length = normed_input.shape[0]
        projected = jnp.dot(normed_input, w_qkv, preferred_element_type=jnp.float32)
        down_projected = jnp.dot(normed_input, adapters, preferred_element_type=jnp.float32).astype(jnp.bfloat16)
        grouped_queries = projected.reshape(sequence_length, KV, QUERY_PER_KV + 2, HD)
        query_rows = (grouped_queries[:, :, :QUERY_PER_KV].reshape(sequence_length, -1) + ADAPTER_SCALE * jnp.dot(down_projected[:, :narrow_rank_rows], query_up_adapter, preferred_element_type=jnp.float32)).astype(jnp.bfloat16)
        key_heads = grouped_queries[:, :, QUERY_PER_KV].reshape(sequence_length, -1).astype(jnp.bfloat16)
        value_rows = (grouped_queries[:, :, QUERY_PER_KV + 1].reshape(sequence_length, -1) + ADAPTER_SCALE * jnp.dot(down_projected[:, narrow_rank_rows:], value_up_adapter, preferred_element_type=jnp.float32)).astype(jnp.bfloat16)
        attended, pullback = jax.vjp(attend, query_rows, key_heads, value_rows)
        query_gradient, grad_keys, value_gradient = pullback(grad_rows)
        query_up_gradient = ADAPTER_SCALE * jnp.einsum('fb,fd->bd', down_projected[:, :narrow_rank_rows], query_gradient, preferred_element_type=jnp.float32)
        value_up_gradient = ADAPTER_SCALE * jnp.einsum('fb,fd->bd', down_projected[:, narrow_rank_rows:], value_gradient, preferred_element_type=jnp.float32)
        middle_gradient = jnp.concatenate([jnp.dot(query_gradient, query_up_adapter.T, preferred_element_type=jnp.float32), jnp.dot(value_gradient, value_up_adapter.T, preferred_element_type=jnp.float32)], 1).astype(jnp.bfloat16)
        down_gradient = ADAPTER_SCALE * jnp.einsum('uh,ux->hx', normed_input, middle_gradient, preferred_element_type=jnp.float32)
        return (attended, down_gradient, query_up_gradient, value_up_gradient)
    attn_out, down_gradient, query_up_gradient, value_up_gradient = lax.map(one_sequence, (tokens, out_grad))
    down_gradient = lax.optimization_barrier(jnp.sum(down_gradient, axis=0))
    return (attn_out, down_gradient[:, :narrow_rank_rows], lax.optimization_barrier(jnp.sum(query_up_gradient, axis=0)), down_gradient[:, narrow_rank_rows:], lax.optimization_barrier(jnp.sum(value_up_gradient, axis=0)))
```

```python
import functools
import math

import jax
import jax.numpy as jnp
from jax import lax
from jax.experimental import pallas as pl
from jax.experimental.pallas import tpu as pltpu
from jax.sharding import PartitionSpec as P

HD = 128
QUERY_PER_KV = 8
LANES = 128
CORES = 2
PIECES = 4

EPSILON = 1e-05
ADAPTER_SCALE = 2.0
ROPE_BASE = 500000.0
MESH = pl.DeviceIdType.MESH


def normalize(own_rows, norm_gain):
    widened = own_rows.astype(jnp.float32)
    mean_square = jnp.mean(widened * widened, axis=-1, keepdims=True)
    return (widened * lax.rsqrt(mean_square + EPSILON) * norm_gain).astype(jnp.bfloat16)


def rotary_tables(sequence_length):
    half_dim = HD // 2
    positions = jnp.arange(sequence_length, dtype=jnp.float32)[:, None]
    inv_freq = ROPE_BASE ** (-jnp.arange(half_dim, dtype=jnp.float32) / half_dim)
    angles = positions * inv_freq
    cosine, sine = jnp.cos(angles), jnp.sin(angles)
    return jnp.concatenate([cosine, cosine], 1), jnp.concatenate([-sine, sine], 1)


def dot(a, b, dims):
    return lax.dot_general(a, b, (dims, ((), ())), preferred_element_type=jnp.float32)


class Place:
    def __init__(self, n, chips, fsdp):
        self.n, self.chips, self.fsdp = n, chips, fsdp
        dp = lax.axis_index("dp")
        self.x, self.c = dp // CORES, lax.rem(dp, CORES)
        self.y, self.z = lax.axis_index("fsdp"), lax.axis_index("tensor")

    def chip(self, a, e):
        return lax.rem(self.x + a, self.chips), lax.rem(self.y + e, self.fsdp)

    def shard(self, a, e, b):
        x, y = self.chip(a, e)
        core = self.c if b == 0 else 1 - self.c
        return (x * CORES + core) * self.fsdp + y

    def plane(self, a, e):
        x, y = self.chip(a, e)
        return x * self.fsdp + y

    def at(self, a, e):
        x, y = self.chip(a, e)
        return {"dp": x * CORES + self.c, "fsdp": y}

    def partner(self):
        return {"dp": self.x * CORES + 1 - self.c}

    def line(self, step):
        return {"tensor": lax.rem(self.z + step, self.n)}

    def others(self):
        return [(a, e) for a in range(self.chips) for e in range(self.fsdp) if (a, e) != (0, 0)]


def remote(src, dst, send, recv, device):
    return pltpu.make_async_remote_copy(
        src_ref=src, dst_ref=dst, send_sem=send, recv_sem=recv, device_id=device, device_id_type=MESH
    )


def greet(devices):
    barrier = pltpu.get_barrier_semaphore()
    for device in devices:
        pl.semaphore_signal(barrier, inc=1, device_id=device, device_id_type=MESH)
    pl.semaphore_wait(barrier, len(devices))


def project_kernel(
    n, chips, fsdp, tok_ref, w_ref, adp_ref, g_ref,
    proj_ref, down_ref, grad_ref,
    wide, blocks, down_sum,
    local_sem, tok_send, tok_recv, g_send, g_recv,
    a1, a2, b1, b2, cross, w_recv,
):
    me = Place(n, chips, fsdp)
    z = me.z
    rows, depth = tok_ref.shape
    shard_rows, cols = w_ref.shape
    half = shard_rows // 2
    span = depth // PIECES
    g_cols = grad_ref.shape[1]

    greet(
        [me.line(s) for s in range(1, n)]
        + [me.at(a, 0) for a in range(1, chips)]
        + [me.at(0, e) for e in range(1, fsdp)]
        + [me.partner()]
    )

    def columns(p):
        return pl.ds(pl.multiple_of(p * span, LANES), span)

    def token_copy(block, p, up, own):
        source = tok_ref.at[:, columns(p)] if own else blocks.at[block, :, columns(p)]
        return remote(
            source, blocks.at[block, :, columns(p)],
            tok_send.at[0 if up else 1, block, p], tok_recv.at[block, p],
            {"tensor": jnp.where(up, jnp.minimum(z + 1, n - 1), jnp.maximum(z - 1, 0))},
        )

    def w_rows(shard, h):
        return pl.ds(pl.multiple_of(shard * shard_rows + h * half, half), half)

    def w_copy(a, e, h, target, sem, own):
        shard = me.shard(a, e, 0)
        place = wide.at[w_rows(shard, h)]
        return remote(
            w_ref.at[pl.ds(h * half, half)] if own else place, place, sem, w_recv.at[shard, h], target
        )

    def w_wait(a, e, b, h):
        shard = me.shard(a, e, b)
        place = wide.at[w_rows(shard, h)]
        remote(place, place, cross.at[0, 0, 0], w_recv.at[shard, h], me.partner()).wait_recv()

    up_ok, down_ok = z < n - 1, z > 0
    for p in range(PIECES):
        @pl.when(up_ok)
        def _():
            token_copy(z, p, True, True).start()

        @pl.when(down_ok)
        def _():
            token_copy(z, p, False, True).start()
    own_w = pltpu.make_async_copy(
        w_ref, wide.at[pl.ds(pl.multiple_of(me.shard(0, 0, 0) * shard_rows, shard_rows), shard_rows)],
        local_sem.at[0],
    )
    own_t = pltpu.make_async_copy(tok_ref, blocks.at[z], local_sem.at[1])
    first_a = [w_copy(0, 0, 0, me.at(0, e), a1.at[e], True) for e in range(1, fsdp)]
    first_b = [w_copy(0, 0, 1, me.at(a, 0), b1.at[a], True) for a in range(1, chips)]
    next_a = [w_copy(0, 0, 0, me.at(a, 0), a2.at[a, 0], True) for a in range(1, chips)]
    next_b = [w_copy(0, 0, 1, me.at(0, e), b2.at[0, e], True) for e in range(1, fsdp)]
    own_cross = [w_copy(0, 0, h, me.partner(), cross.at[0, 0, h], True) for h in range(2)]
    w_sent = first_a + first_b + next_a + next_b + own_cross
    for copy in w_sent:
        copy.start()
    own_t.start()
    own_w.start()

    proj_ref[...] = jnp.zeros_like(proj_ref)
    down_sum[...] = jnp.zeros_like(down_sum)

    grads = []
    for s in range(1, n):
        to = lax.rem(z + s, n)
        grads.append(remote(
            g_ref.at[:, pl.ds(pl.multiple_of(to * g_cols, g_cols), g_cols)],
            grad_ref.at[pl.ds(pl.multiple_of(z * rows, rows), rows)],
            g_send.at[s], g_recv.at[s], me.line(s),
        ))
    for copy in grads:
        copy.start()
    own_g = pltpu.make_async_copy(
        g_ref.at[:, pl.ds(pl.multiple_of(z * g_cols, g_cols), g_cols)],
        grad_ref.at[pl.ds(pl.multiple_of(z * rows, rows), rows)], local_sem.at[2],
    )
    own_g.start()

    def pass_on(copies):
        for copy in copies:
            copy.start()
            w_sent.append(copy)

    for e in range(1, fsdp):
        w_wait(0, e, 0, 0)
        pass_on([w_copy(0, e, 0, me.at(a, 0), a2.at[a, e], False) for a in range(1, chips)])
        pass_on([w_copy(0, e, 0, me.partner(), cross.at[0, e, 0], False)])
    for a in range(1, chips):
        w_wait(a, 0, 0, 1)
        pass_on([w_copy(a, 0, 1, me.at(0, e), b2.at[a, e], False) for e in range(1, fsdp)])
        pass_on([w_copy(a, 0, 1, me.partner(), cross.at[a, 0, 1], False)])
    for a in range(1, chips):
        w_wait(a, 0, 0, 0)
        pass_on([w_copy(a, 0, 0, me.partner(), cross.at[a, 0, 0], False)])
    for e in range(1, fsdp):
        w_wait(0, e, 0, 1)
        pass_on([w_copy(0, e, 1, me.partner(), cross.at[0, e, 1], False)])

    def arrive(block, p, up):
        token_copy(block, p, up, False).wait_recv()

        @pl.when(up_ok if up else down_ok)
        def _():
            token_copy(block, p, up, False).start()

    def arrive_both(s, p):
        @pl.when(z - s >= 0)
        def _():
            arrive(jnp.maximum(z - s, 0), p, True)

        @pl.when(z + s <= n - 1)
        def _():
            arrive(jnp.minimum(z + s, n - 1), p, False)

    width = 2 * LANES

    def multiply(block, p):
        at_rows = pl.ds(pl.multiple_of(block * rows, rows), rows)
        deep = pl.ds(pl.multiple_of(p * span, span), span)

        @pl.loop(0, cols // width)
        def _(tile):
            lanes = pl.ds(pl.multiple_of(tile * width, width), width)
            proj_ref[at_rows, lanes] += dot(blocks[block, :, columns(p)], wide[deep, lanes], ((1,), (0,)))

        down_sum[at_rows, :] += dot(blocks[block, :, columns(p)], adp_ref[deep, :], ((1,), (0,)))

    for p in range(PIECES):
        arrive_both(1, p)
    for a in range(1, chips):
        for e in range(1, fsdp):
            for h in range(2):
                w_wait(a, e, 0, h)
                pass_on([w_copy(a, e, h, me.partner(), cross.at[a, e, h], False)])
    for a in range(chips):
        for e in range(fsdp):
            for h in range(2):
                w_wait(a, e, 1, h)
    own_w.wait()
    own_t.wait()

    @pl.loop(0, PIECES)
    def _(p):
        multiply(z, p)

    for s in range(1, n):
        @pl.loop(0, PIECES)
        def _(p):
            @pl.when(z - s >= 0)
            def _():
                multiply(jnp.maximum(z - s, 0), p)

            @pl.when(z + s <= n - 1)
            def _():
                multiply(jnp.minimum(z + s, n - 1), p)

            if s + 1 < n:
                arrive_both(s + 1, p)

    down_ref[...] = down_sum[...].astype(jnp.bfloat16)

    own_g.wait()
    for copy in grads:
        copy.wait()
    for copy in w_sent:
        copy.wait_send()

    @pl.loop(0, PIECES)
    def _(p):
        @pl.when(up_ok)
        def _():
            token_copy(z, p, True, True).wait_send()

        @pl.when(down_ok)
        def _():
            token_copy(z, p, False, True).wait_send()

        for s in range(1, n):
            @pl.when((z - s >= 0) & up_ok)
            def _():
                token_copy(jnp.maximum(z - s, 0), p, True, False).wait_send()

            @pl.when((z + s <= n - 1) & down_ok)
            def _():
                token_copy(jnp.minimum(z + s, n - 1), p, False, False).wait_send()


def project(sizes, own, w_qkv, adapters, out_grad):
    n, chips, fsdp = sizes
    rows, depth = own.shape
    shard_rows, cols = w_qkv.shape
    g_cols = out_grad.shape[1] // n
    shards = chips * CORES * fsdp
    dma = pltpu.SemaphoreType.DMA
    anywhere = pl.BlockSpec(memory_space=pl.ANY)
    vmem = pl.BlockSpec(memory_space=pltpu.VMEM)
    return pl.pallas_call(
        functools.partial(project_kernel, n, chips, fsdp),
        in_specs=[anywhere, anywhere, vmem, anywhere],
        out_specs=[vmem, vmem, anywhere],
        out_shape=[
            jax.ShapeDtypeStruct((n * rows, cols), jnp.float32),
            jax.ShapeDtypeStruct((n * rows, LANES), jnp.bfloat16),
            jax.ShapeDtypeStruct((n * rows, g_cols), jnp.bfloat16),
        ],
        scratch_shapes=[
            pltpu.VMEM((depth, cols), jnp.bfloat16),
            pltpu.VMEM((n, rows, depth), jnp.bfloat16),
            pltpu.VMEM((n * rows, LANES), jnp.float32),
            dma((3,)),
            dma((2, n, PIECES)),
            dma((n, PIECES)),
            dma((n,)),
            dma((n,)),
            dma((fsdp,)),
            dma((chips, fsdp)),
            dma((chips,)),
            dma((chips, fsdp)),
            dma((chips, fsdp, 2)),
            dma((shards, 2)),
        ],
        compiler_params=pltpu.CompilerParams(
            collective_id=0, has_side_effects=True, vmem_limit_bytes=60 * 2**20
        ),
        cost_estimate=pl.CostEstimate(
            flops=2 * n * rows * depth * cols, bytes_accessed=depth * cols * 2, transcendentals=0
        ),
        name="project",
    )(own, w_qkv, adapters, out_grad)


def attention_kernel(
    block, n, q_ref, k_ref, v_ref, dq_ref, dv_ref, qup_ref, vup_ref, cos_ref, sin_ref, g_ref,
    out_ref, gbq_ref, gbv_ref, mid_ref,
    keys, values, value_grad, query_grad, staged, send_sem, recv_sem, local_sem,
):
    group, head = pl.program_id(0), pl.program_id(1)
    groups, heads = pl.num_programs(0), pl.num_programs(1)
    length = q_ref.shape[0]
    rows_each = length // n
    rank = qup_ref.shape[0]
    scale = 1.0 / math.sqrt(HD)
    z = lax.axis_index("tensor")
    index = group * heads + head

    @pl.when(index == 0)
    def _():
        greet([{"tensor": lax.rem(z + s, n)} for s in range(1, n)])
        mid_ref[...] = jnp.zeros_like(mid_ref)

    @pl.when(head == 0)
    def _():
        k = k_ref[...].astype(jnp.bfloat16).astype(jnp.float32)
        keys[...] = (k * cos_ref[...] + pltpu.roll(k, HD // 2, 1) * sin_ref[...]).astype(jnp.bfloat16)
        values[...] = (
            v_ref[...] + ADAPTER_SCALE * dot(dv_ref[...], vup_ref[...], ((1,), (0,)))
        ).astype(jnp.bfloat16)
        value_grad[...] = jnp.zeros_like(value_grad)

    for start in range(0, length, block):
        rows = pl.ds(start, block)
        reach = start + block
        q = (
            q_ref[rows, :] + ADAPTER_SCALE * dot(dq_ref[rows, :], qup_ref[...], ((1,), (0,)))
        ).astype(jnp.bfloat16).astype(jnp.float32)
        cosine, sine = cos_ref[rows, :], sin_ref[rows, :]
        turned = (q * cosine + pltpu.roll(q, HD // 2, 1) * sine).astype(jnp.bfloat16)
        k, v, g = keys[pl.ds(0, reach), :], values[pl.ds(0, reach), :], g_ref[rows, :]
        scores = dot(turned, k, ((1,), (1,))) * scale
        row = lax.broadcasted_iota(jnp.int32, scores.shape, 0) + start
        col = lax.broadcasted_iota(jnp.int32, scores.shape, 1)
        scores = jnp.where(row >= col, scores, -1e30)
        weights = jnp.exp(scores - jnp.max(scores, axis=-1, keepdims=True))
        wide = weights * (1.0 / jnp.sum(weights, axis=-1, keepdims=True))
        probabilities = wide.astype(jnp.bfloat16)
        staged[index, rows, :] = dot(probabilities, v, ((1,), (0,))).astype(jnp.bfloat16)
        value_grad[pl.ds(0, reach), :] += dot(probabilities, g, ((0,), (0,)))
        prob_grad = dot(g, v, ((1,), (1,)))
        inner = jnp.sum(prob_grad * wide, axis=-1, keepdims=True)
        score_grad = (wide * (prob_grad - inner) * scale).astype(jnp.bfloat16)
        turned_grad = dot(score_grad, k, ((1,), (0,))).astype(jnp.bfloat16).astype(jnp.float32)
        query_grad[rows, :] = (
            turned_grad * cosine - pltpu.roll(turned_grad, HD // 2, 1) * sine
        ).astype(jnp.bfloat16)

    gq = query_grad[...]
    gbq_ref[...] = ADAPTER_SCALE * dot(dq_ref[...], gq, ((0,), (0,)))
    mid_ref[:, pl.ds(0, rank)] += dot(gq, qup_ref[...], ((1,), (1,)))

    @pl.when(head == heads - 1)
    def _():
        gv = value_grad[...].astype(jnp.bfloat16)
        gbv_ref[...] = ADAPTER_SCALE * dot(dv_ref[...], gv, ((0,), (0,)))
        mid_ref[:, pl.ds(rank, rank)] += dot(gv, vup_ref[...], ((1,), (1,)))

    def columns(which, owner):
        return pl.ds(pl.multiple_of((owner * groups * heads + which) * HD, HD), HD)

    def copies(which):
        found = []
        for s in range(1, n):
            to = lax.rem(z + s, n)
            found.append(remote(
                staged.at[which, pl.ds(pl.multiple_of(to * rows_each, rows_each), rows_each)],
                out_ref.at[:, columns(which, z)],
                send_sem.at[s, which], recv_sem.at[s, which], {"tensor": to},
            ))
        mine = pltpu.make_async_copy(
            staged.at[which, pl.ds(pl.multiple_of(z * rows_each, rows_each), rows_each)],
            out_ref.at[:, columns(which, z)], local_sem.at[which],
        )
        return found, mine

    found, mine = copies(index)
    for copy in found:
        copy.start()
    mine.start()

    @pl.when(index == groups * heads - 1)
    def _():
        @pl.loop(0, groups * heads)
        def _(which):
            found, mine = copies(which)
            for copy in found:
                copy.wait()
            mine.wait()


def attention(n, projected, down_q, down_v, query_up, value_up, grad_rows):
    length, cols = projected.shape
    rank = down_q.shape[1]
    per = QUERY_PER_KV + 2
    groups = cols // (per * HD)
    block = 256 if length % 256 == 0 else length
    cosine, sine = rotary_tables(length)
    heads = groups * QUERY_PER_KV
    whole = lambda shape: pl.BlockSpec(shape, lambda g, h: (0, 0))
    column = lambda n, index: pl.BlockSpec((n, HD), lambda g, h: (0, index(g, h)))
    by_head = lambda g, h: g * QUERY_PER_KV + h
    return pl.pallas_call(
        functools.partial(attention_kernel, block, n),
        grid=(groups, QUERY_PER_KV),
        in_specs=[
            column(length, lambda g, h: g * per + h),
            column(length, lambda g, h: g * per + QUERY_PER_KV),
            column(length, lambda g, h: g * per + QUERY_PER_KV + 1),
            whole((length, rank)),
            whole((length, rank)),
            column(rank, by_head),
            column(rank, lambda g, h: g),
            whole((length, HD)),
            whole((length, HD)),
            column(length, by_head),
        ],
        out_specs=[
            pl.BlockSpec(memory_space=pl.ANY),
            column(rank, by_head),
            column(rank, lambda g, h: g),
            whole((length, LANES)),
        ],
        out_shape=[
            jax.ShapeDtypeStruct((length // n, n * heads * HD), jnp.bfloat16),
            jax.ShapeDtypeStruct((rank, heads * HD), jnp.float32),
            jax.ShapeDtypeStruct((rank, groups * HD), jnp.float32),
            jax.ShapeDtypeStruct((length, LANES), jnp.float32),
        ],
        scratch_shapes=[
            pltpu.VMEM((length, HD), jnp.bfloat16),
            pltpu.VMEM((length, HD), jnp.bfloat16),
            pltpu.VMEM((length, HD), jnp.float32),
            pltpu.VMEM((length, HD), jnp.bfloat16),
            pltpu.VMEM((heads, length, HD), jnp.bfloat16),
            pltpu.SemaphoreType.DMA((n, heads)),
            pltpu.SemaphoreType.DMA((n, heads)),
            pltpu.SemaphoreType.DMA((heads,)),
        ],
        compiler_params=pltpu.CompilerParams(
            dimension_semantics=("arbitrary", "arbitrary"), vmem_limit_bytes=48 * 2**20,
            collective_id=1, has_side_effects=True,
        ),
        cost_estimate=pl.CostEstimate(
            flops=10 * heads * length * length * HD,
            bytes_accessed=length * cols * 4 + 2 * length * heads * HD * 2,
            transcendentals=heads * length * length,
        ),
        name="attention",
    )(projected, projected, projected, down_q, down_v, query_up, value_up, cosine, sine, grad_rows)


def finish_kernel(
    n, chips, fsdp, mid_ref, own_ref, gb_ref,
    down_ref, gbo_ref,
    mid_in, mid_own, part, part_in, spread, spread_in, line_sum, line_in, line_all, kept, other,
    gb_in, gb_all,
    mid_s, mid_r, core_s, core_r, plane_s, plane_r, line_s, line_r, all_s, all_r, keep_s, keep_r,
    gbp_s, gbp_r,
):
    me = Place(n, chips, fsdp)
    z, c = me.z, me.c
    rows, depth = own_ref.shape
    height = part.shape[1]
    count = chips * fsdp
    piece = spread.shape[2]
    tall = height // n
    gb_half = gb_ref.shape[0] // CORES
    here = me.plane(0, 0)
    others = me.others()
    greet([me.line(s) for s in range(1, n)] + [me.at(a, e) for a, e in others] + [me.partner()])

    def mid_rows(t):
        return pl.ds(pl.multiple_of(t * rows, rows), rows)

    def gb_rows(core):
        return pl.ds(pl.multiple_of(core * gb_half, gb_half), gb_half)

    def line_rows(t):
        return pl.ds(pl.multiple_of(t * tall, tall), tall)

    mids = [
        remote(mid_ref.at[mid_rows(lax.rem(z + s, n))], mid_in.at[s], mid_s.at[s], mid_r.at[s], me.line(s))
        for s in range(1, n)
    ]
    for copy in mids:
        copy.start()
    gb_core = remote(gb_ref.at[gb_rows(1 - c)], gb_in, core_s.at[1], core_r.at[1], me.partner())
    gb_core.start()

    total = mid_ref[mid_rows(z), :]
    for s, copy in zip(range(1, n), mids):
        copy.wait()
        total = total + mid_in[s]
    mid_own[...] = total.astype(jnp.bfloat16)

    width = 4 * LANES

    def product(core):
        @pl.loop(0, depth // 2 // width)
        def _(tile):
            lanes = pl.ds(pl.multiple_of(tile * width, width), width)
            source = pl.ds(pl.multiple_of(core * (depth // 2) + tile * width, width), width)
            whole = dot(mid_own[...], own_ref[:, source], ((0,), (0,)))
            part[core, :, lanes] = ADAPTER_SCALE * whole[:height]

    product(1 - c)
    core_copy = remote(part.at[1 - c], part_in, core_s.at[0], core_r.at[0], me.partner())
    core_copy.start()
    product(c)

    gb_core.wait()
    gb_all[here] = gb_ref[gb_rows(c), :] + gb_in[...]
    gb_plane = [
        remote(gb_all.at[here], gb_all.at[here], gbp_s.at[i], gbp_r.at[here], me.at(a, e))
        for i, (a, e) in enumerate(others)
    ]
    core_copy.wait()
    for k in range(count):
        lanes = pl.ds(k * piece, piece)
        summed = part[c, :, lanes] + part_in[:, lanes]
        part[c, :, lanes] = summed
        spread[k] = summed.astype(jnp.bfloat16)
    planes = []
    for i, (a, e) in enumerate(others):
        planes.append(remote(
            spread.at[me.plane(a, e)], spread_in.at[here], plane_s.at[i], plane_r.at[here], me.at(a, e)
        ))
        planes[-1].start()
    for copy in gb_plane:
        copy.start()

    def plane_wait(buffer, sems, a, e):
        source = me.plane(a, e)
        remote(buffer.at[source], buffer.at[source], plane_s.at[0], sems.at[source], me.at(a, e)).wait_recv()

    summed = part[c, :, pl.ds(pl.multiple_of(here * piece, piece), piece)]
    for a, e in others:
        plane_wait(spread_in, plane_r, a, e)
        summed = summed + spread_in[me.plane(a, e)].astype(jnp.float32)
    line_sum[...] = summed
    lines = [
        remote(line_sum.at[line_rows(lax.rem(z + s, n))], line_in.at[s], line_s.at[s], line_r.at[s], me.line(s))
        for s in range(1, n)
    ]
    for copy in lines:
        copy.start()
    summed = line_sum[line_rows(z), :]
    for s, copy in zip(range(1, n), lines):
        copy.wait_recv()
        summed = summed + line_in[s]
    line_all[line_rows(z), :] = summed
    alls = [
        remote(line_all.at[line_rows(z)], line_all.at[line_rows(z)], all_s.at[s], all_r.at[s], me.line(s))
        for s in range(1, n)
    ]
    for copy in alls:
        copy.start()

    for a, e in others:
        plane_wait(gb_all, gbp_r, a, e)
    gb_sum = gb_all[0]
    for k in range(1, count):
        gb_sum = gb_sum + gb_all[k]
    gbo_ref[gb_rows(c), :] = gb_sum
    gb_back = remote(gbo_ref.at[gb_rows(c)], gbo_ref.at[gb_rows(c)], core_s.at[2], core_r.at[2], me.partner())
    gb_back.start()

    for s in range(1, n):
        source = lax.rem(z + n - s, n)
        remote(
            line_all.at[line_rows(source)], line_all.at[line_rows(source)], all_s.at[s], all_r.at[s], me.line(s)
        ).wait_recv()
    kept[here] = line_all[...].astype(jnp.bfloat16)
    keeps = [
        remote(kept.at[here], kept.at[here], keep_s.at[i], keep_r.at[here], me.at(a, e))
        for i, (a, e) in enumerate(others)
    ]
    for copy in keeps:
        copy.start()
    for a, e in others:
        plane_wait(kept, keep_r, a, e)
    back = remote(kept, other, core_s.at[3], core_r.at[3], me.partner())
    back.start()

    def put(buffer, core):
        for k in range(count):
            start = pl.multiple_of(core * (depth // 2) + k * piece, piece)
            down_ref[:, pl.ds(start, piece)] = buffer[k].astype(jnp.float32)

    put(kept, c)
    back.wait()
    put(other, 1 - c)
    gb_back.wait_send()
    remote(
        gbo_ref.at[gb_rows(1 - c)], gbo_ref.at[gb_rows(1 - c)], core_s.at[2], core_r.at[2], me.partner()
    ).wait_recv()
    for copy in planes + gb_plane + lines + alls + keeps:
        copy.wait_send()


def finish(sizes, mid, own, gb, height):
    n, chips, fsdp = sizes
    rows, depth = own.shape
    count = chips * fsdp
    piece = depth // CORES // count
    dma = pltpu.SemaphoreType.DMA
    vmem = pl.BlockSpec(memory_space=pltpu.VMEM)
    f32, bf16 = jnp.float32, jnp.bfloat16
    return pl.pallas_call(
        functools.partial(finish_kernel, n, chips, fsdp),
        in_specs=[vmem] * 3,
        out_specs=[vmem] * 2,
        out_shape=[jax.ShapeDtypeStruct((height, depth), f32), jax.ShapeDtypeStruct(gb.shape, f32)],
        scratch_shapes=[
            pltpu.VMEM((n, rows, LANES), f32),
            pltpu.VMEM((rows, LANES), bf16),
            pltpu.VMEM((CORES, height, depth // CORES), f32),
            pltpu.VMEM((height, depth // CORES), f32),
            pltpu.VMEM((count, height, piece), bf16),
            pltpu.VMEM((count, height, piece), bf16),
            pltpu.VMEM((height, piece), f32),
            pltpu.VMEM((n, height // n, piece), f32),
            pltpu.VMEM((height, piece), f32),
            pltpu.VMEM((count, height, piece), bf16),
            pltpu.VMEM((count, height, piece), bf16),
            pltpu.VMEM((gb.shape[0] // CORES, gb.shape[1]), f32),
            pltpu.VMEM((count, gb.shape[0] // CORES, gb.shape[1]), f32),
            dma((n,)), dma((n,)),
            dma((4,)), dma((4,)),
            dma((count,)), dma((count,)),
            dma((n,)), dma((n,)),
            dma((n,)), dma((n,)),
            dma((count,)), dma((count,)),
            dma((count,)), dma((count,)),
        ],
        compiler_params=pltpu.CompilerParams(
            collective_id=2, has_side_effects=True, vmem_limit_bytes=32 * 2**20
        ),
        cost_estimate=pl.CostEstimate(
            flops=2 * rows * depth * LANES, bytes_accessed=rows * depth * 2, transcendentals=0
        ),
        name="finish",
    )(mid, own, gb)


def local(sizes, tokens, norm_gain, w_qkv, a_query, query_up_adapter, a_value, value_up_adapter, out_grad):
    n = sizes[0]
    own = normalize(tokens[0], norm_gain)
    rank = a_query.shape[1]
    depth = own.shape[1]
    adapters = jnp.concatenate(
        [a_query, a_value, jnp.zeros((depth, LANES - 2 * rank), a_query.dtype)], 1
    )
    projected, down_projected, grad_rows = project(sizes, own, w_qkv, adapters, out_grad[0])
    out_rows, query_up_gradient, value_up_gradient, mid = attention(
        n, projected, down_projected[:, :rank], down_projected[:, rank:2 * rank],
        query_up_adapter, value_up_adapter, grad_rows,
    )
    query_cols = query_up_gradient.shape[1]
    down_gradient, up_gradient = finish(
        sizes, mid, own, jnp.concatenate([query_up_gradient, value_up_gradient], 1), 2 * rank
    )
    down_gradient = down_gradient.T
    return (
        out_rows[None],
        down_gradient[:, :rank],
        up_gradient[:, :query_cols],
        down_gradient[:, rank:],
        up_gradient[:, query_cols:],
    )


def solution(mesh):
    sizes = (mesh.shape["tensor"], mesh.shape["dp"] // CORES, mesh.shape["fsdp"])
    return jax.shard_map(
        functools.partial(local, sizes),
        mesh=mesh,
        in_specs=(
            P(("dp", "fsdp"), "tensor", None),
            P(),
            P(("dp", "fsdp"), "tensor"),
            P(),
            P(None, "tensor"),
            P(),
            P(None, "tensor"),
            P(("dp", "fsdp"), "tensor", None),
        ),
        out_specs=(
            P(("dp", "fsdp"), "tensor", None),
            P(),
            P(None, "tensor"),
            P(),
            P(None, "tensor"),
        ),
        check_vma=False,
    )
```
